256 devices in a mesh: row: 32 (over y, z), col: 8 (over x, core).
Axes of the slice: x: 4, y: 4, z: 8, core: 2. Of those that a mesh axis runs over, the one named last changes fastest.
Arguments:
- sim_window: bfloat16 [6144, 6144], P('row', 'col'), as said below
- sim_rest: bfloat16 [6144, 113856], P('row', 'col'), may hold values from -6 to 6
- joined_partner_pairs: int32 [768, 2], replicated, may hold values from 0 to 6143, as said below
- cluster_member_count: int32 [6144], replicated, may hold values from 1 to 64
Outputs:
- window_out: bfloat16 [6144, 6144], P('row', 'col')
- rest_out: bfloat16 [6144, 113856], P('row', 'col')
The draws below stay inside these ranges and needn't reach their ends.
Inputs may be any that keep to these rules, and one draw needn't show every extreme that they name: `joined_partner_pairs`: each row is (survivor, partner); no window item appears twice in the whole list. Each aligned block of 192 items holds exactly 24 partners. For any two aligned blocks (possibly the same), at most 3 pairs have their partner in the first and their survivor in the second, and some two blocks have exactly 3. Nearly symmetric: sim_window[i, j] is close to sim_window[j, i].
All inputs are finite; a program needn't handle non-finite values.
Results may differ from the reference program's by a relative error of at most 0.001.
Values may be sent and summed in bfloat16 or wider, within the bound.
No kernel may reach another device: no remote copies, remote signals or barrier semaphores. Data moves between devices by JAX's collectives and lax.ppermute only.
A program may use at most 128 MiB of HBM per device.

```python
import jax
import jax.numpy as jnp
from jax import lax

WINDOW_PER_ROW = 192
PARTNERS_PER_ROW = 24
CAP = 3
M = 6144
PAIRS = 768
REST = 113856


def block_shuffle(subkey):
    return jax.random.permutation(subkey, WINDOW_PER_ROW)


def draw_joined_partner_pairs(key, part):
    block_total = M // WINDOW_PER_ROW
    subkeys = jax.random.split(key, 3)
    block_order = jax.random.permutation(subkeys[0], block_total)
    hot_blocks = block_order[:4]
    cold_blocks = block_order[4:]
    pair_ids = jnp.arange(PAIRS, dtype=jnp.int32)
    src_index = pair_ids // PARTNERS_PER_ROW
    slot_index = pair_ids % PARTNERS_PER_ROW
    half_width = PARTNERS_PER_ROW // 2
    hot_dst = hot_blocks[jnp.minimum(slot_index // CAP, 3)]
    cold_dst = cold_blocks[(src_index + slot_index - half_width) % (block_total - 4)]
    destination_block = jnp.where(slot_index < half_width, hot_dst, cold_dst)
    row_permutations = jax.vmap(block_shuffle)(jax.random.split(subkeys[1], block_total))
    vanishing_node = src_index * WINDOW_PER_ROW + row_permutations[src_index, slot_index]
    one_hot = (destination_block[:, None] == jnp.arange(block_total, dtype=jnp.int32)[None, :]).astype(jnp.int32)
    incoming_entry = jnp.sum((jnp.cumsum(one_hot, axis=0) - one_hot) * one_hot, axis=1)
    lasting_node = destination_block * WINDOW_PER_ROW + row_permutations[destination_block, PARTNERS_PER_ROW + incoming_entry]
    reorder_indices = jax.random.permutation(subkeys[2], PAIRS)
    return jnp.stack([lasting_node, vanishing_node], axis=1)[reorder_indices].astype(jnp.int32)


def draw_sim_window(key, part):
    base = jax.random.normal(key, (M, M), jnp.float32)
    symmetric = (base + base.T) * 0.70710678
    return symmetric.astype(jnp.bfloat16)


def with_ends(values, key, low, high):
    longest = values.shape.index(max(values.shape))
    spots = []
    for shift in (0, 1):
        where = [jax.random.randint(jax.random.fold_in(key, axis), (), 0, length) for axis, length in enumerate(values.shape)]
        where[longest] = (where[longest] + shift) % values.shape[longest]
        spots.append(tuple(where))
    return values.at[spots[0]].set(low).at[spots[1]].set(high)


def shard_levels(stream_key, dims, shards, least, top_value):
    level, own = 1.0, jax.random.fold_in(stream_key, 6)
    for dim, parts in shards:
        steps = jnp.exp(jax.random.uniform(jax.random.fold_in(own, dim), (parts,), jnp.float32, least / len(shards), top_value / len(shards)))
        level = level * jnp.repeat(steps, dims[dim] // parts).reshape([-1 if axis == dim else 1 for axis in range(len(dims))])
    return level


def gaussian(own_key, dims, scale, limit, cuts=(), held_as=jnp.bfloat16):
    array = jax.random.normal(own_key, dims, jnp.float32) * scale
    if len(cuts) > 0:
        array = shard_levels(own_key, dims, cuts, -0.22, 0.18) * array
    return jnp.clip(array, min=-limit, max=limit).astype(held_as)


def setup_inputs(seed: int = 0) -> dict:
    streams_of = jax.random.split(jax.random.key(seed), 5)
    sim_window = draw_sim_window(jax.random.fold_in(streams_of[4], 71), 0)
    sim_rest = gaussian(streams_of[1], (M, REST), 1.0, 6.0, ((0, 32), (1, 8)))
    joined_partner_pairs = draw_joined_partner_pairs(jax.random.fold_in(streams_of[4], 71), 0)
    cluster_member_count = with_ends(jax.random.randint(streams_of[3], (M,), 1, 65), jax.random.fold_in(streams_of[3], 1), 1, 64).astype(jnp.int32)
    return dict(sim_window=sim_window, sim_rest=sim_rest, joined_partner_pairs=joined_partner_pairs, cluster_member_count=cluster_member_count)


def merge_weights(joined_partner_pairs, cluster_member_count):
    lasting_node = joined_partner_pairs[:, 0]
    vanishing_node = joined_partner_pairs[:, 1]
    remaining_size = cluster_member_count[lasting_node].astype(jnp.float32)
    absorbed_size = cluster_member_count[vanishing_node].astype(jnp.float32)
    joined_cluster_size = remaining_size + absorbed_size
    item_grand_sum = cluster_member_count.shape[0]
    retained_entries = jnp.ones((item_grand_sum,), jnp.float32).at[lasting_node].set(remaining_size / joined_cluster_size).at[vanishing_node].set(0.0)
    selected_entries = jnp.zeros((item_grand_sum,), jnp.float32).at[lasting_node].set(absorbed_size / joined_cluster_size)
    donor_position = jnp.zeros((item_grand_sum,), jnp.int32).at[lasting_node].set(vanishing_node.astype(jnp.int32))
    return retained_entries, selected_entries, donor_position


def combine_rows(matrix, retained_entries, selected_entries, donor_position):
    row_total = matrix.shape[0]
    block_rows = 128
    starts = jnp.arange(row_total // block_rows, dtype=jnp.int32) * block_rows

    def one_block(offset):
        own_rows = lax.dynamic_slice_in_dim(matrix, offset, block_rows, 0).astype(jnp.float32)
        source_ids = lax.dynamic_slice_in_dim(donor_position, offset, block_rows, 0).astype(jnp.int32)
        partner_rows = matrix[source_ids].astype(jnp.float32)
        keep_block = lax.dynamic_slice_in_dim(retained_entries, offset, block_rows, 0)
        take_block = lax.dynamic_slice_in_dim(selected_entries, offset, block_rows, 0)
        return (keep_block[:, None] * own_rows + take_block[:, None] * partner_rows).astype(jnp.bfloat16)

    blocks_out = lax.map(one_block, starts)
    return blocks_out.reshape(row_total, matrix.shape[1])


def reference(sim_window, sim_rest, joined_partner_pairs, cluster_member_count):
    retained_entries, selected_entries, donor_position = merge_weights(joined_partner_pairs, cluster_member_count)
    mixed_window = combine_rows(sim_window, retained_entries, selected_entries, donor_position)
    rest_out = combine_rows(sim_rest, retained_entries, selected_entries, donor_position)
    window_out = combine_rows(mixed_window.T, retained_entries, selected_entries, donor_position).T
    return window_out, rest_out
```

```python
import functools

import jax
import jax.numpy as jnp
from jax import lax
from jax.experimental import pallas as pl
from jax.experimental.pallas import tpu as pltpu
from jax.sharding import PartitionSpec as P


NY, NZ = 4, 8
SEND = 24
CAP = 3
HOPS = (24, 24, 18, 6)
HOP_BASE = (0, 24, 48, 66)
ONE_WAY = sum(HOPS)
OWN = CAP * NY
PIECES = 4
WIDTH = 1280
SLOTS = NY * NZ * CAP
BF = jnp.bfloat16
F32 = jnp.float32


def row_perm(dy, dz):
    return [
        (y * NZ + z, (y + dy) % NY * NZ + (z + dz) % NZ) for y in range(NY) for z in range(NZ)
    ]


def hot(ids, count, on=None):
    mask = ids[None, :] == jnp.arange(count, dtype=jnp.int32)[:, None]
    if on is not None:
        mask = mask & on[None, :]
    return mask.astype(BF)


def hot4(ids, count, on=None):
    mask = ids[None, :] == (jnp.arange(count * PIECES, dtype=jnp.int32) // PIECES)[:, None]
    if on is not None:
        mask = mask & on[None, :]
    return mask.astype(BF)


def join(left, right):
    return lax.dot_general(left, right, (((1,), (1,)), ((), ())), preferred_element_type=F32).astype(BF)


def rank(code):
    order = jnp.arange(code.shape[0], dtype=jnp.int32)
    same = (code[None, :] == code[:, None]) & (order[None, :] < order[:, None])
    return jnp.sum(same.astype(jnp.int32), axis=1)


def item_weights(labels, lasting, vanishing, retained_pair, selected_pair):
    is_last = labels[:, None] == lasting[None, :]
    is_gone = labels[:, None] == vanishing[None, :]
    matched = jnp.sum((is_last | is_gone).astype(F32), axis=1)
    keep = 1.0 - matched + jnp.sum(jnp.where(is_last, retained_pair[None, :], 0.0), axis=1)
    take = jnp.sum(jnp.where(is_last, selected_pair[None, :], 0.0), axis=1)
    return keep, take


def sizes_of(items, counts2d):
    rows = hot(items // 128, counts2d.shape[0])
    lines = lax.dot_general(rows, counts2d, (((0,), (0,)), ((), ())), preferred_element_type=F32)
    lane = (items % 128)[:, None] == jnp.arange(128, dtype=jnp.int32)[None, :]
    return jnp.sum(jnp.where(lane, lines, 0.0), axis=1)


def select_kernel(with_window, *refs):
    if with_window:
        sel, x0, x1, x2, x3, win, cw, ccw, own, last = refs
        last[...] = x3[...]
        last[:, 256:1024] = win[...]
        blocks = (x0, x1, x2, last)
    else:
        sel, x0, x1, x2, x3, cw, ccw, own = refs
        blocks = (x0, x1, x2, x3)
    s = sel[...]
    piece = lax.broadcasted_iota(jnp.int32, s.shape, 0) % PIECES
    parts = [jnp.where(piece == q, s, jnp.zeros_like(s)) for q in range(PIECES)]
    n = SEND * PIECES

    @pl.loop(0, WIDTH // 256)
    def _(t):
        cols = pl.ds(pl.multiple_of(t * 256, 256), 256)
        acc = jnp.dot(parts[0], blocks[0][:, cols], preferred_element_type=F32)
        for q in range(1, PIECES):
            acc += jnp.dot(parts[q], blocks[q][:, cols], preferred_element_type=F32)
        out = acc.astype(BF)
        cw[:, cols] = out[:n]
        ccw[:, cols] = out[n : 2 * n]
        own[:, cols] = out[2 * n :]


def select(sel, rest, window, first_block):
    rows = rest.shape[0]
    full = lambda shape: pl.BlockSpec(shape, lambda i: (0, 0))
    block = lambda b: pl.BlockSpec((rows, WIDTH), lambda i: (0, b))
    shapes = [(SEND * PIECES, WIDTH)] * 2 + [(OWN * PIECES, WIDTH)]
    with_window = window is not None
    return pl.pallas_call(
        functools.partial(select_kernel, with_window),
        grid=(1,),
        in_specs=[full(sel.shape)]
        + [block(first_block + q) for q in range(PIECES)]
        + ([full(window.shape)] if with_window else []),
        out_specs=[full(s) for s in shapes],
        out_shape=[jax.ShapeDtypeStruct(s, BF) for s in shapes],
        scratch_shapes=[pltpu.VMEM((rows, WIDTH), BF)] if with_window else [],
        cost_estimate=pl.CostEstimate(
            flops=2 * sel.shape[0] * rows * PIECES * WIDTH,
            bytes_accessed=2 * rows * PIECES * WIDTH,
            transcendentals=0,
        ),
        name="select",
    )(sel, *([rest] * PIECES), *([window] if with_window else []))


def turn_kernel(count, *refs):
    sel, parts, outs, stack = refs[0], refs[1 : 1 + count], refs[1 + count : -1], refs[-1]
    at = 0
    for part in parts:
        stack[at : at + part.shape[0], :] = part[...]
        at += part.shape[0]
    n = SEND * PIECES

    @pl.loop(0, WIDTH // 256)
    def _(t):
        cols = pl.ds(pl.multiple_of(t * 256, 256), 256)
        out = jnp.dot(sel[...], stack[:, cols], preferred_element_type=F32).astype(BF)
        for dy in range(NY):
            outs[dy][:, cols] = out[dy * n : (dy + 1) * n]


def turn(sel, parts):
    full = lambda shape: pl.BlockSpec(shape, lambda i: (0, 0))
    shape = (SEND * PIECES, WIDTH)
    return pl.pallas_call(
        functools.partial(turn_kernel, len(parts)),
        grid=(1,),
        in_specs=[full(sel.shape)] + [full(p.shape) for p in parts],
        out_specs=[full(shape)] * NY,
        out_shape=[jax.ShapeDtypeStruct(shape, BF)] * NY,
        scratch_shapes=[pltpu.VMEM((sel.shape[1], WIDTH), BF)],
        cost_estimate=pl.CostEstimate(
            flops=2 * sel.shape[0] * sel.shape[1] * WIDTH, bytes_accessed=sel.size * 2, transcendentals=0
        ),
        name="turn",
    )(sel, *parts)


def blend_kernel(with_window, aliased, *refs):
    place, keep, take, y0, y1, y2, y3, x = refs[:8]
    refs = refs[8:]
    if with_window:
        win, refs = refs[0], refs[1:]
    if aliased:
        refs = refs[1:]
    if with_window:
        out, mixed, stack = refs
    else:
        out, stack = refs
    q = pl.program_id(0)
    n = SEND * PIECES

    @pl.when(q == 0)
    def _():
        for dy, y in enumerate((y0, y1, y2, y3)):
            stack[dy * n : (dy + 1) * n, :] = y[...]

    p = place[...]
    p = jnp.where(lax.broadcasted_iota(jnp.int32, p.shape, 1) % PIECES == q, p, jnp.zeros_like(p))
    k, t = keep[...], take[...]

    @pl.loop(0, WIDTH // 256)
    def _(i):
        cols = pl.ds(pl.multiple_of(i * 256, 256), 256)
        placed = jnp.dot(p, stack[:, cols], preferred_element_type=F32)
        out[:, cols] = (k * x[:, cols].astype(F32) + t * placed).astype(BF)

    if with_window:

        @pl.when(q == PIECES - 1)
        def _():
            for i in range(3):
                placed = jnp.dot(p, stack[:, 256 + 256 * i : 512 + 256 * i], preferred_element_type=F32)
                own = win[:, 256 * i : 256 * i + 256].astype(F32)
                mixed[:, 256 * i : 256 * i + 256] = (k * own + t * placed).astype(BF)


def blend(place, keep, take, ys, rest, window, first_block, into):
    rows = rest.shape[0]
    full = lambda shape: pl.BlockSpec(shape, lambda q: (0, 0))
    block = pl.BlockSpec((rows, WIDTH), lambda q: (0, first_block + q))
    with_window, aliased = window is not None, into is not None
    args = [place, keep, take, *ys, rest]
    in_specs = [full(a.shape) for a in args[:-1]] + [block]
    out_shape, out_specs = [jax.ShapeDtypeStruct(rest.shape, BF)], [block]
    if with_window:
        args.append(window)
        in_specs.append(full(window.shape))
        out_shape.append(jax.ShapeDtypeStruct(window.shape, BF))
        out_specs.append(full(window.shape))
    if aliased:
        args.append(into)
        in_specs.append(pl.BlockSpec(memory_space=pl.ANY))
    return pl.pallas_call(
        functools.partial(blend_kernel, with_window, aliased),
        grid=(PIECES,),
        in_specs=in_specs,
        out_specs=out_specs,
        out_shape=out_shape,
        scratch_shapes=[pltpu.VMEM((SLOTS * PIECES, WIDTH), BF)],
        input_output_aliases={len(args) - 1: 0} if aliased else {},
        cost_estimate=pl.CostEstimate(
            flops=2 * place.shape[0] * place.shape[1] * PIECES * WIDTH,
            bytes_accessed=4 * rows * PIECES * WIDTH,
            transcendentals=0,
        ),
        name="blend",
    )(*args)


def shards(sim_window, sim_rest, joined_partner_pairs, cluster_member_count):
    rows, wcols = sim_window.shape
    me, my_col = lax.axis_index("row"), lax.axis_index("col")
    cols_n = lax.axis_size("col")
    my_y, my_z = me // NZ, me % NZ
    last, gone = joined_partner_pairs[:, 0], joined_partner_pairs[:, 1]
    src, dst = gone // rows, last // rows
    src_y, src_z, dst_y, dst_z = src // NZ, src % NZ, dst // NZ, dst % NZ
    order = jnp.arange(last.shape[0], dtype=jnp.int32)

    ahead = (dst_z - src_z) % NZ
    up = (ahead > 0) & ((ahead < 4) | ((ahead == 4) & (rank(src * NZ + ahead) % 2 == 0)))
    way = jnp.where(ahead == 0, 2, jnp.where(up, 0, 1))
    dist = jnp.where(up, ahead, (NZ - ahead) % NZ)
    base = (src * 3 + way) * 8192
    key = base + (7 - dist) * 1024 + order
    pos = jnp.sum(
        ((key[None, :] >= base[:, None]) & (key[None, :] < key[:, None])).astype(jnp.int32), axis=1
    )
    sel = join(hot4(way * SEND + pos, 2 * SEND + OWN, src == me), hot(gone - me * rows, rows))

    hop_base = jnp.where(dist < 2, HOP_BASE[0], jnp.where(dist == 2, HOP_BASE[1], jnp.where(dist == 3, HOP_BASE[2], HOP_BASE[3])))
    found = jnp.where(way == 2, 2 * ONE_WAY + pos, way * ONE_WAY + hop_base + pos)
    slot = (dst_y - src_y) % NY * (NZ * CAP) + src_z * CAP + rank(src * (NY * NZ) + dst)
    turning = join(
        hot4(slot, SLOTS, (src_y == my_y) & (dst_z == my_z)), hot4(found, 2 * ONE_WAY + OWN)
    )
    piece_r = jnp.arange(turning.shape[0], dtype=jnp.int32) % PIECES
    piece_c = jnp.arange(turning.shape[1], dtype=jnp.int32) % PIECES
    turning = jnp.where(piece_r[:, None] == piece_c[None, :], turning, jnp.zeros_like(turning))
    place = join(hot(last - me * rows, rows, dst == me), hot4(slot, SLOTS))

    counts2d = cluster_member_count.astype(BF).reshape(-1, 128)
    size_last, size_gone = sizes_of(last, counts2d), sizes_of(gone, counts2d)
    retained, selected = size_last / (size_last + size_gone), size_gone / (size_last + size_gone)
    keep, take = item_weights(
        me * rows + jnp.arange(rows, dtype=jnp.int32), last, gone, retained, selected
    )
    keep, take = keep[:, None], take[:, None]

    into = None
    for chunk, first_block in enumerate((8, 0, 4)):
        window = sim_window if chunk == 0 else None
        up_list, down_list, own_list = select(sel, sim_rest, window, first_block)
        parts = []
        for step, rows_now in ((1, up_list), (-1, down_list)):
            for hops in HOPS:
                rows_now = lax.ppermute(rows_now[: hops * PIECES], "row", row_perm(0, step))
                parts.append(rows_now)
        parts.append(own_list)
        ys = turn(turning, parts)
        ys = [ys[0]] + [lax.ppermute(ys[dy], "row", row_perm(dy, 0)) for dy in range(1, NY)]
        outs = blend(place, keep, take, ys, sim_rest, window, first_block, into)
        if chunk == 0:
            mixed = outs[1]
        into = outs[0]

    gone_col, last_col = gone // wcols, last // wcols
    col_rank = rank(gone_col)
    lane = 128
    pick = join(hot(gone - my_col * wcols, wcols), hot(col_rank, lane, gone_col == my_col))
    mine = jnp.dot(mixed, pick, preferred_element_type=F32).astype(BF)
    pieces = [mine] + [
        lax.ppermute(mine, "col", [(c, (c + k) % cols_n) for c in range(cols_n)]) for k in range(1, cols_n)
    ]
    spread = join(
        hot((my_col - gone_col) % cols_n * lane + col_rank, cols_n * lane), hot(last - my_col * wcols, wcols)
    )
    gathered = jnp.dot(jnp.concatenate(pieces, axis=1), spread, preferred_element_type=F32)
    ckeep, ctake = item_weights(
        my_col * wcols + jnp.arange(wcols, dtype=jnp.int32), last, gone, retained, selected
    )
    window_out = (ckeep[None, :] * mixed.astype(F32) + ctake[None, :] * gathered).astype(BF)
    return window_out, into


def solution(mesh):
    in_specs = (P("row", "col"), P("row", "col"), P(), P())
    out_specs = (P("row", "col"), P("row", "col"))
    return jax.shard_map(shards, mesh=mesh, in_specs=in_specs, out_specs=out_specs, check_vma=False)
```

```python
import functools

import jax
import jax.numpy as jnp
from jax import lax
from jax.experimental import pallas as pl
from jax.experimental.pallas import tpu as pltpu
from jax.sharding import PartitionSpec as P


NY, NZ = 4, 8
SEND = 24
CAP = 3
HOPS = (24, 24, 16, 8)
HOP_BASE = (0, 24, 48, 64)
ONE_WAY = sum(HOPS)
OWN = 16
SLOTS = NY * NZ * CAP
BLOCK = 1280
TILE = 256
EDGE = 256
CHUNKS = ((7, 11), (3, 7), (0, 3))
BF = jnp.bfloat16
F32 = jnp.float32
VMEM = pl.BlockSpec(memory_space=pltpu.VMEM)
ANY = pl.BlockSpec(memory_space=pl.ANY)


def row_perm(dy, dz):
    return [
        (y * NZ + z, (y + dy) % NY * NZ + (z + dz) % NZ) for y in range(NY) for z in range(NZ)
    ]


def hot(ids, count, on=None):
    mask = ids[None, :] == jnp.arange(count, dtype=jnp.int32)[:, None]
    if on is not None:
        mask = mask & on[None, :]
    return mask.astype(BF)


def join(left, right):
    return lax.dot_general(left, right, (((1,), (1,)), ((), ())), preferred_element_type=F32).astype(BF)


def rank(code):
    order = jnp.arange(code.shape[0], dtype=jnp.int32)
    same = (code[None, :] == code[:, None]) & (order[None, :] < order[:, None])
    return jnp.sum(same.astype(jnp.int32), axis=1)


def item_weights(labels, lasting, vanishing, retained_pair, selected_pair):
    is_last = labels[:, None] == lasting[None, :]
    is_gone = labels[:, None] == vanishing[None, :]
    matched = jnp.sum((is_last | is_gone).astype(F32), axis=1)
    keep = 1.0 - matched + jnp.sum(jnp.where(is_last, retained_pair[None, :], 0.0), axis=1)
    take = jnp.sum(jnp.where(is_last, selected_pair[None, :], 0.0), axis=1)
    return keep, take


def sizes_of(items, counts2d):
    rows = hot(items // 128, counts2d.shape[0])
    lines = lax.dot_general(rows, counts2d, (((0,), (0,)), ((), ())), preferred_element_type=F32)
    lane = (items % 128)[:, None] == jnp.arange(128, dtype=jnp.int32)[None, :]
    return jnp.sum(jnp.where(lane, lines, 0.0), axis=1)


def params(limit_mib):
    return pltpu.CompilerParams(vmem_limit_bytes=limit_mib * 1024 * 1024)


def tiles(start, width, body):
    @pl.loop(0, width // TILE)
    def _(t):
        body(pl.ds(pl.multiple_of(start + t * TILE, TILE), TILE))


def edge_pieces(rest, start):
    tail = rest.shape[1] - start
    whole = tail // 128 * 128
    return [(at, width) for at, width in ((0, whole), (whole, tail - whole)) if width]


def select_kernel(first, last, *refs):
    if len(refs) == 6:
        sel, rest, win, up, down, own = refs
    else:
        sel, rest, up, down, own = refs

    def put(x, cols):
        out = jnp.dot(sel[...], x, preferred_element_type=F32).astype(BF)
        up[:, cols] = out[:SEND]
        down[:, cols] = out[SEND : 2 * SEND]
        own[:, cols] = out[2 * SEND :]

    width = (last - first) * BLOCK

    @pl.loop(0, width // TILE)
    def _(t):
        at = pl.multiple_of(t * TILE, TILE)
        put(rest[:, pl.ds(pl.multiple_of(first * BLOCK + at, TILE), TILE)], pl.ds(at, TILE))

    if len(refs) == 6:
        whole = rest.shape[1] // BLOCK * BLOCK
        for at, n in edge_pieces(rest, whole):
            put(rest[:, whole + at : whole + at + n], pl.ds(width + at, n))
        for at in range(0, win.shape[1], TILE):
            put(win[:, at : at + TILE], pl.ds(width + EDGE + at, TILE))


def select(sel, rest, side, first, last):
    rows = rest.shape[0]
    width = (last - first) * BLOCK + sum(EDGE + s.shape[1] for s in side)
    shapes = [(SEND, width), (SEND, width), (OWN, width)]
    return pl.pallas_call(
        functools.partial(select_kernel, first, last),
        in_specs=[VMEM] * (2 + len(side)),
        out_specs=[VMEM] * 3,
        out_shape=[jax.ShapeDtypeStruct(s, BF) for s in shapes],
        compiler_params=params(16),
        cost_estimate=pl.CostEstimate(
            flops=2 * sel.shape[0] * rows * width, bytes_accessed=2 * rows * width, transcendentals=0
        ),
        name="select",
    )(sel, rest, *side)


def weights_kernel(first_row, last, gone, retained, selected, keep, take):
    rows = keep.shape[0]
    label = first_row[0] + lax.broadcasted_iota(jnp.int32, (rows, last.shape[1]), 0)
    is_last, is_gone = label == last[...], label == gone[...]
    kept = jnp.where(is_last, retained[...], jnp.where(is_gone, 0.0, 1.0))
    keep[...] = jnp.min(kept, axis=1, keepdims=True)
    take[...] = jnp.max(jnp.where(is_last, selected[...], 0.0), axis=1, keepdims=True)


def row_weights(first_row, rows, last, gone, retained, selected):
    return pl.pallas_call(
        weights_kernel,
        in_specs=[pl.BlockSpec(memory_space=pltpu.SMEM)] + [VMEM] * 4,
        out_specs=[VMEM] * 2,
        out_shape=[jax.ShapeDtypeStruct((rows, 1), F32)] * 2,
        compiler_params=params(4),
        cost_estimate=pl.CostEstimate(flops=8 * rows * last.shape[0], bytes_accessed=0, transcendentals=0),
        name="row_weights",
    )(first_row[None], last[None, :], gone[None, :], retained[None, :], selected[None, :])


def stack_rows(stack, parts, cols):
    at = 0
    for part in parts:
        stack[at : at + part.shape[0], cols] = part[:, cols]
        at += part.shape[0]


def turn_kernel(count, *refs):
    sel, parts, outs, stack = refs[0], refs[1 : 1 + count], refs[1 + count : -1], refs[-1]

    def body(cols):
        stack_rows(stack, parts, cols)
        out = jnp.dot(sel[...], stack[:, cols], preferred_element_type=F32).astype(BF)
        for dy in range(NY):
            outs[dy][:, cols] = out[dy * SEND : (dy + 1) * SEND]

    tiles(0, stack.shape[1], body)


def turn(sel, parts):
    width = parts[0].shape[1]
    return pl.pallas_call(
        functools.partial(turn_kernel, len(parts)),
        in_specs=[VMEM] * (1 + len(parts)),
        out_specs=[VMEM] * NY,
        out_shape=[jax.ShapeDtypeStruct((SEND, width), BF)] * NY,
        scratch_shapes=[pltpu.VMEM((sel.shape[1], width), BF)],
        compiler_params=params(8),
        cost_estimate=pl.CostEstimate(
            flops=2 * sel.shape[0] * sel.shape[1] * width, bytes_accessed=sel.size * 2, transcendentals=0
        ),
        name="turn",
    )(sel, *parts)


def blend_kernel(first, last, with_side, aliased, *refs):
    place, keep, take, y0, y1, y2, y3, rest = refs[:8]
    refs = refs[8:]
    if with_side:
        win, pick = refs[:2]
        refs = refs[2:]
    refs = refs[aliased:]
    if with_side:
        out, edge, mixed, mine, stack, done, sems = refs
    else:
        out, stack, done, sems = refs
    ys = (y0, y1, y2, y3)
    k, t = keep[...], take[...]

    def value(x, cols):
        stack_rows(stack, ys, cols)
        placed = jnp.dot(place[...], stack[:, cols], preferred_element_type=F32)
        return (k * x.astype(F32) + t * placed).astype(BF)

    copies = []
    for i, b in enumerate(range(first, last)):

        def body(cols, shift=first * BLOCK):
            done[:, cols] = value(rest[:, pl.ds(pl.multiple_of(shift + cols.start, TILE), TILE)], cols)

        tiles(i * BLOCK, BLOCK, body)
        here = pl.ds(i * BLOCK, BLOCK)
        copies.append(
            pltpu.make_async_copy(done.at[:, here], out.at[:, b * BLOCK : (b + 1) * BLOCK], sems.at[i])
        )
        copies[-1].start()
    if with_side:
        side = (last - first) * BLOCK
        whole = rest.shape[1] // BLOCK * BLOCK
        for at, n in edge_pieces(rest, whole):
            edge[:, at : at + n] = value(rest[:, whole + at : whole + at + n], pl.ds(side + at, n))
        for at in range(0, mixed.shape[1], TILE):
            mixed[:, at : at + TILE] = value(win[:, at : at + TILE], pl.ds(side + EDGE + at, TILE))
        mine[...] = jnp.dot(mixed[...], pick[...], preferred_element_type=F32).astype(BF)
    for copy in copies:
        copy.wait()


def blend(place, keep, take, ys, rest, first, last, side, into):
    rows, total = rest.shape
    width = ys[0].shape[1]
    with_side, aliased = bool(side), into is not None
    args = [place, keep, take, *ys, rest, *side] + ([into] if aliased else [])
    out_shape, out_specs = [jax.ShapeDtypeStruct((rows, total), BF)], [ANY]
    if with_side:
        out_shape += [jax.ShapeDtypeStruct((rows, n), BF) for n in (EDGE, side[0].shape[1], side[1].shape[1])]
        out_specs += [VMEM] * 3
    return pl.pallas_call(
        functools.partial(blend_kernel, first, last, with_side, aliased),
        in_specs=[VMEM] * (8 + len(side)) + [ANY] * aliased,
        out_specs=out_specs,
        out_shape=out_shape,
        scratch_shapes=[
            pltpu.VMEM((SLOTS, width), BF),
            pltpu.VMEM((rows, (last - first) * BLOCK), BF),
            pltpu.SemaphoreType.DMA((last - first,)),
        ],
        input_output_aliases={len(args) - 1: 0} if aliased else {},
        compiler_params=params(16),
        cost_estimate=pl.CostEstimate(
            flops=4 * place.shape[0] * place.shape[1] * width,
            bytes_accessed=2 * rows * width,
            transcendentals=0,
        ),
        name="blend",
    )(*args)


def columns_kernel(mixed, keep, take, spread, p0, p1, p2, p3, out, stack, done, sem):
    rows = mixed.shape[0]
    at = 0
    for p in (p0, p1, p2, p3):
        for i in range(p.shape[0] // rows):
            stack[:, at * 128 : (at + 1) * 128] = p[i * rows : (i + 1) * rows, :]
            at += 1

    def body(cols):
        got = jnp.dot(stack[...], spread[:, cols], preferred_element_type=F32)
        done[:, cols] = (keep[:, cols] * mixed[:, cols].astype(F32) + take[:, cols] * got).astype(BF)

    tiles(0, mixed.shape[1], body)
    copy = pltpu.make_async_copy(done, out, sem)
    copy.start()
    copy.wait()


def columns(mixed, keep, take, spread, pieces):
    return pl.pallas_call(
        columns_kernel,
        in_specs=[VMEM] * 8,
        out_specs=ANY,
        out_shape=jax.ShapeDtypeStruct(mixed.shape, BF),
        scratch_shapes=[
            pltpu.VMEM((mixed.shape[0], spread.shape[0]), BF),
            pltpu.VMEM(mixed.shape, BF),
            pltpu.SemaphoreType.DMA,
        ],
        compiler_params=params(8),
        cost_estimate=pl.CostEstimate(
            flops=2 * mixed.size * spread.shape[0], bytes_accessed=2 * mixed.size, transcendentals=0
        ),
        name="columns",
    )(mixed, keep, take, spread, *pieces)


def shards(sim_window, sim_rest, joined_partner_pairs, cluster_member_count):
    rows, wcols = sim_window.shape
    total = sim_rest.shape[1]
    me, my_col = lax.axis_index("row"), lax.axis_index("col")
    cols_n = lax.axis_size("col")
    my_y, my_z = me // NZ, me % NZ
    last, gone = joined_partner_pairs[:, 0], joined_partner_pairs[:, 1]
    src, dst = gone // rows, last // rows
    src_y, src_z, dst_y, dst_z = src // NZ, src % NZ, dst // NZ, dst % NZ
    order = jnp.arange(last.shape[0], dtype=jnp.int32)

    ahead = (dst_z - src_z) % NZ
    three = jnp.sum(((src[None, :] == src[:, None]) & (ahead == 3)[None, :]).astype(jnp.int32), axis=1)
    four_up = (ahead == 4) & (rank(src * NZ + ahead) < jnp.minimum(HOPS[3], HOPS[2] - three))
    up = ((ahead > 0) & (ahead < 4)) | four_up
    way = jnp.where(ahead == 0, 2, jnp.where(up, 0, 1))
    dist = jnp.where(up, ahead, (NZ - ahead) % NZ)
    base = (src * 3 + way) * 8192
    key = base + (7 - dist) * 1024 + order
    pos = jnp.sum(
        ((key[None, :] >= base[:, None]) & (key[None, :] < key[:, None])).astype(jnp.int32), axis=1
    )
    sel = join(hot(way * SEND + pos, 2 * SEND + OWN, src == me), hot(gone - me * rows, rows))

    hop_base = jnp.where(
        dist < 2, HOP_BASE[0], jnp.where(dist == 2, HOP_BASE[1], jnp.where(dist == 3, HOP_BASE[2], HOP_BASE[3]))
    )
    found = jnp.where(way == 2, 2 * ONE_WAY + pos, way * ONE_WAY + hop_base + pos)
    slot = (dst_y - src_y) % NY * (NZ * CAP) + src_z * CAP + rank(src * (NY * NZ) + dst)
    turning = join(
        hot(slot, SLOTS, (src_y == my_y) & (dst_z == my_z)), hot(found, 2 * ONE_WAY + OWN)
    )
    place = join(hot(last - me * rows, rows, dst == me), hot(slot, SLOTS))

    counts2d = cluster_member_count.astype(BF).reshape(-1, 128)
    size_last, size_gone = sizes_of(last, counts2d), sizes_of(gone, counts2d)
    retained, selected = size_last / (size_last + size_gone), size_gone / (size_last + size_gone)
    keep, take = row_weights(me * rows, rows, last, gone, retained, selected)
    gone_col, last_col = gone // wcols, last // wcols
    col_rank = rank(gone_col)
    lane = 128
    pick = join(hot(gone - my_col * wcols, wcols), hot(col_rank, lane, gone_col == my_col))

    whole = total // BLOCK * BLOCK
    into = None
    for chunk, (first, end) in enumerate(CHUNKS):
        side = (sim_window,) if chunk == 0 else ()
        up_list, down_list, own_list = select(sel, sim_rest, side, first, end)
        parts = []
        for step, rows_now in ((1, up_list), (-1, down_list)):
            for hops in HOPS:
                rows_now = lax.ppermute(rows_now[:hops], "row", row_perm(0, step))
                parts.append(rows_now)
        parts.append(own_list)
        ys = turn(turning, parts)
        ys = [ys[0]] + [lax.ppermute(ys[dy], "row", row_perm(dy, 0)) for dy in range(1, NY)]
        if side:
            side = (sim_window, pick)
        outs = blend(place, keep, take, ys, sim_rest, first, end, side, into)
        into = outs[0]
        if side:
            into = lax.dynamic_update_slice(into, outs[1][:, : total - whole], (0, whole))
            mixed, mine = outs[2:]

    pieces = [mine]
    step = 1
    while step < cols_n:
        held = jnp.concatenate(pieces, axis=0)
        pieces.append(lax.ppermute(held, "col", [(c, c ^ step) for c in range(cols_n)]))
        step *= 2
    spread = join(
        hot((my_col ^ gone_col) * lane + col_rank, cols_n * lane), hot(last - my_col * wcols, wcols)
    )
    ckeep, ctake = item_weights(
        my_col * wcols + jnp.arange(wcols, dtype=jnp.int32), last, gone, retained, selected
    )
    window_out = columns(mixed, ckeep[None, :], ctake[None, :], spread, pieces)
    return window_out, into


def solution(mesh):
    in_specs = (P("row", "col"), P("row", "col"), P(), P())
    out_specs = (P("row", "col"), P("row", "col"))
    return jax.shard_map(shards, mesh=mesh, in_specs=in_specs, out_specs=out_specs, check_vma=False)
```

```python
import functools

import jax
import jax.numpy as jnp
from jax import lax
from jax.experimental import pallas as pl
from jax.experimental.pallas import tpu as pltpu
from jax.sharding import PartitionSpec as P


NY, NZ = 4, 8
SEND = 24
CAP = 3
HOPS = (24, 24, 16, 8)
HOP_BASE = (0, 24, 48, 64)
ONE_WAY = sum(HOPS)
OWN = 16
SLOTS = NY * NZ * CAP
BLOCK = 1280
TILE = 256
EDGE = 256
CHUNKS = ((6, 11), (0, 6))
BF = jnp.bfloat16
F32 = jnp.float32
VMEM = pl.BlockSpec(memory_space=pltpu.VMEM)
ANY = pl.BlockSpec(memory_space=pl.ANY)
HBM = pl.BlockSpec(memory_space=pltpu.HBM)


def row_perm(dy, dz):
    return [
        (y * NZ + z, (y + dy) % NY * NZ + (z + dz) % NZ) for y in range(NY) for z in range(NZ)
    ]


def hot(ids, count, on=None):
    mask = ids[None, :] == jnp.arange(count, dtype=jnp.int32)[:, None]
    if on is not None:
        mask = mask & on[None, :]
    return mask.astype(BF)


def join(left, right):
    return lax.dot_general(left, right, (((1,), (1,)), ((), ())), preferred_element_type=F32).astype(BF)


def rank(code):
    order = jnp.arange(code.shape[0], dtype=jnp.int32)
    same = (code[None, :] == code[:, None]) & (order[None, :] < order[:, None])
    return jnp.sum(same.astype(jnp.int32), axis=1)


def item_weights(labels, lasting, vanishing, retained_pair, selected_pair):
    is_last = labels[:, None] == lasting[None, :]
    is_gone = labels[:, None] == vanishing[None, :]
    matched = jnp.sum((is_last | is_gone).astype(F32), axis=1)
    keep = 1.0 - matched + jnp.sum(jnp.where(is_last, retained_pair[None, :], 0.0), axis=1)
    take = jnp.sum(jnp.where(is_last, selected_pair[None, :], 0.0), axis=1)
    return keep, take


def sizes_of(items, counts2d):
    rows = hot(items // 128, counts2d.shape[0])
    lines = lax.dot_general(rows, counts2d, (((0,), (0,)), ((), ())), preferred_element_type=F32)
    lane = (items % 128)[:, None] == jnp.arange(128, dtype=jnp.int32)[None, :]
    return jnp.sum(jnp.where(lane, lines, 0.0), axis=1)


def params(limit_mib):
    return pltpu.CompilerParams(vmem_limit_bytes=limit_mib * 1024 * 1024)


def tiles(start, width, body):
    @pl.loop(0, width // TILE, unroll=5)
    def _(t):
        body(pl.ds(pl.multiple_of(start + t * TILE, TILE), TILE))


def edge_pieces(rest, start):
    tail = rest.shape[1] - start
    whole = tail // 128 * 128
    return [(at, width) for at, width in ((0, whole), (whole, tail - whole)) if width]


def select_kernel(first, last, with_side, *refs):
    if with_side:
        sel, rest, edge, win, up, down, own, held, sems = refs
    else:
        sel, rest, up, down, own, held, sems = refs
    copies = []
    for i, b in enumerate(range(first, last)):
        copies.append((rest.at[:, b * BLOCK : (b + 1) * BLOCK], i * BLOCK, BLOCK))
    if with_side:
        side = (last - first) * BLOCK
        copies.append((win, side + EDGE, win.shape[1]))
    started = []
    for i, (ref, at, width) in enumerate(copies):
        started.append(pltpu.make_async_copy(ref, held.at[:, at : at + width], sems.at[i]))
        started[-1].start()

    def put(cols):
        out = jnp.dot(sel[...], held[:, cols], preferred_element_type=F32).astype(BF)
        up[:, cols] = out[:SEND]
        down[:, cols] = out[SEND : 2 * SEND]
        own[:, cols] = out[2 * SEND :]

    if with_side:
        held[:, side : side + EDGE] = edge[...]
        put(pl.ds(side, EDGE))
    for copy, (_, at, width) in zip(started, copies):
        copy.wait()
        tiles(at, width, put)


def select(sel, rest, side, first, last):
    rows = rest.shape[0]
    width = (last - first) * BLOCK + sum(s.shape[1] for s in side)
    shapes = [(SEND, width), (SEND, width), (OWN, width)]
    return pl.pallas_call(
        functools.partial(select_kernel, first, last, bool(side)),
        in_specs=[VMEM, HBM] + ([VMEM, HBM] if side else []),
        out_specs=[VMEM] * 3,
        out_shape=[jax.ShapeDtypeStruct(s, BF) for s in shapes],
        scratch_shapes=[pltpu.VMEM((rows, width), BF), pltpu.SemaphoreType.DMA((last - first + 1,))],
        compiler_params=params(55 if side else 51),
        cost_estimate=pl.CostEstimate(
            flops=2 * sel.shape[0] * rows * width, bytes_accessed=2 * rows * width, transcendentals=0
        ),
        name="select",
    )(sel, rest, *side)


def weights_kernel(first_row, last, gone, retained, selected, keep, take):
    rows = keep.shape[0]
    label = first_row[0] + lax.broadcasted_iota(jnp.int32, (rows, last.shape[1]), 0)
    is_last, is_gone = label == last[...], label == gone[...]
    kept = jnp.where(is_last, retained[...], jnp.where(is_gone, 0.0, 1.0))
    keep[...] = jnp.min(kept, axis=1, keepdims=True)
    take[...] = jnp.max(jnp.where(is_last, selected[...], 0.0), axis=1, keepdims=True)


def row_weights(first_row, rows, last, gone, retained, selected):
    return pl.pallas_call(
        weights_kernel,
        in_specs=[pl.BlockSpec(memory_space=pltpu.SMEM)] + [VMEM] * 4,
        out_specs=[VMEM] * 2,
        out_shape=[jax.ShapeDtypeStruct((rows, 1), F32)] * 2,
        compiler_params=params(4),
        cost_estimate=pl.CostEstimate(flops=8 * rows * last.shape[0], bytes_accessed=0, transcendentals=0),
        name="row_weights",
    )(first_row[None], last[None, :], gone[None, :], retained[None, :], selected[None, :])


def stack_rows(stack, parts, cols):
    at = 0
    for part in parts:
        stack[at : at + part.shape[0], cols] = part[:, cols]
        at += part.shape[0]


def turn_kernel(count, *refs):
    sel, parts, outs, stack = refs[0], refs[1 : 1 + count], refs[1 + count : -1], refs[-1]

    def body(cols):
        stack_rows(stack, parts, cols)
        out = jnp.dot(sel[...], stack[:, cols], preferred_element_type=F32).astype(BF)
        for dy in range(NY):
            outs[dy][:, cols] = out[dy * SEND : (dy + 1) * SEND]

    tiles(0, stack.shape[1], body)


def turn(sel, parts):
    width = parts[0].shape[1]
    return pl.pallas_call(
        functools.partial(turn_kernel, len(parts)),
        in_specs=[VMEM] * (1 + len(parts)),
        out_specs=[VMEM] * NY,
        out_shape=[jax.ShapeDtypeStruct((SEND, width), BF)] * NY,
        scratch_shapes=[pltpu.VMEM((sel.shape[1], width), BF)],
        compiler_params=params(8),
        cost_estimate=pl.CostEstimate(
            flops=2 * sel.shape[0] * sel.shape[1] * width, bytes_accessed=sel.size * 2, transcendentals=0
        ),
        name="turn",
    )(sel, *parts)


def blend_kernel(first, last, with_side, aliased, *refs):
    place, keep, take, y0, y1, y2, y3, rest = refs[:8]
    refs = refs[8:]
    if with_side:
        win, pick = refs[:2]
        refs = refs[2:]
    refs = refs[aliased:]
    if with_side:
        out, edge, mixed, mine, stack, done, sems = refs
    else:
        out, stack, done, sems = refs
    ys = (y0, y1, y2, y3)
    k, t = keep[...], take[...]

    def value(x, cols):
        stack_rows(stack, ys, cols)
        placed = jnp.dot(place[...], stack[:, cols], preferred_element_type=F32)
        return (k * x.astype(F32) + t * placed).astype(BF)

    copies = []
    for i, b in enumerate(range(first, last)):

        def body(cols, shift=first * BLOCK):
            done[:, cols] = value(rest[:, pl.ds(pl.multiple_of(shift + cols.start, TILE), TILE)], cols)

        tiles(i * BLOCK, BLOCK, body)
        here = pl.ds(i * BLOCK, BLOCK)
        copies.append(
            pltpu.make_async_copy(done.at[:, here], out.at[:, b * BLOCK : (b + 1) * BLOCK], sems.at[i])
        )
        copies[-1].start()
    if with_side:
        side = (last - first) * BLOCK
        whole = rest.shape[1] // BLOCK * BLOCK
        for at, n in edge_pieces(rest, whole):
            edge[:, at : at + n] = value(rest[:, whole + at : whole + at + n], pl.ds(side + at, n))
        for at in range(0, mixed.shape[1], TILE):
            mixed[:, at : at + TILE] = value(win[:, at : at + TILE], pl.ds(side + EDGE + at, TILE))
        mine[...] = jnp.dot(mixed[...], pick[...], preferred_element_type=F32).astype(BF)
    for copy in copies:
        copy.wait()


def blend(place, keep, take, ys, rest, first, last, side, into):
    rows, total = rest.shape
    width = ys[0].shape[1]
    with_side, aliased = bool(side), into is not None
    args = [place, keep, take, *ys, rest, *side] + ([into] if aliased else [])
    out_shape, out_specs = [jax.ShapeDtypeStruct((rows, total), BF)], [ANY]
    if with_side:
        out_shape += [jax.ShapeDtypeStruct((rows, n), BF) for n in (EDGE, side[0].shape[1], side[1].shape[1])]
        out_specs += [VMEM] * 3
    return pl.pallas_call(
        functools.partial(blend_kernel, first, last, with_side, aliased),
        in_specs=[VMEM] * (8 + len(side)) + [ANY] * aliased,
        out_specs=out_specs,
        out_shape=out_shape,
        scratch_shapes=[
            pltpu.VMEM((SLOTS, width), BF),
            pltpu.VMEM((rows, (last - first) * BLOCK), BF),
            pltpu.SemaphoreType.DMA((last - first,)),
        ],
        input_output_aliases={len(args) - 1: 0} if aliased else {},
        compiler_params=params(16),
        cost_estimate=pl.CostEstimate(
            flops=4 * place.shape[0] * place.shape[1] * width,
            bytes_accessed=2 * rows * width,
            transcendentals=0,
        ),
        name="blend",
    )(*args)


def columns_kernel(mixed, keep, take, spread, p0, p1, p2, p3, out, stack, done, sem):
    rows = mixed.shape[0]
    at = 0
    for p in (p0, p1, p2, p3):
        for i in range(p.shape[0] // rows):
            stack[:, at * 128 : (at + 1) * 128] = p[i * rows : (i + 1) * rows, :]
            at += 1

    def body(cols):
        got = jnp.dot(stack[...], spread[:, cols], preferred_element_type=F32)
        done[:, cols] = (keep[:, cols] * mixed[:, cols].astype(F32) + take[:, cols] * got).astype(BF)

    tiles(0, mixed.shape[1], body)
    copy = pltpu.make_async_copy(done, out, sem)
    copy.start()
    copy.wait()


def columns(mixed, keep, take, spread, pieces):
    return pl.pallas_call(
        columns_kernel,
        in_specs=[VMEM] * 8,
        out_specs=ANY,
        out_shape=jax.ShapeDtypeStruct(mixed.shape, BF),
        scratch_shapes=[
            pltpu.VMEM((mixed.shape[0], spread.shape[0]), BF),
            pltpu.VMEM(mixed.shape, BF),
            pltpu.SemaphoreType.DMA,
        ],
        compiler_params=params(8),
        cost_estimate=pl.CostEstimate(
            flops=2 * mixed.size * spread.shape[0], bytes_accessed=2 * mixed.size, transcendentals=0
        ),
        name="columns",
    )(mixed, keep, take, spread, *pieces)


def shards(sim_window, sim_rest, joined_partner_pairs, cluster_member_count):
    rows, wcols = sim_window.shape
    total = sim_rest.shape[1]
    me, my_col = lax.axis_index("row"), lax.axis_index("col")
    cols_n = lax.axis_size("col")
    my_y, my_z = me // NZ, me % NZ
    last, gone = joined_partner_pairs[:, 0], joined_partner_pairs[:, 1]
    src, dst = gone // rows, last // rows
    src_y, src_z, dst_y, dst_z = src // NZ, src % NZ, dst // NZ, dst % NZ
    order = jnp.arange(last.shape[0], dtype=jnp.int32)

    ahead = (dst_z - src_z) % NZ
    three = jnp.sum(((src[None, :] == src[:, None]) & (ahead == 3)[None, :]).astype(jnp.int32), axis=1)
    four_up = (ahead == 4) & (rank(src * NZ + ahead) < jnp.minimum(HOPS[3], HOPS[2] - three))
    up = ((ahead > 0) & (ahead < 4)) | four_up
    way = jnp.where(ahead == 0, 2, jnp.where(up, 0, 1))
    dist = jnp.where(up, ahead, (NZ - ahead) % NZ)
    base = (src * 3 + way) * 8192
    key = base + (7 - dist) * 1024 + order
    pos = jnp.sum(
        ((key[None, :] >= base[:, None]) & (key[None, :] < key[:, None])).astype(jnp.int32), axis=1
    )
    sel = join(hot(way * SEND + pos, 2 * SEND + OWN, src == me), hot(gone - me * rows, rows))

    hop_base = jnp.where(
        dist < 2, HOP_BASE[0], jnp.where(dist == 2, HOP_BASE[1], jnp.where(dist == 3, HOP_BASE[2], HOP_BASE[3]))
    )
    found = jnp.where(way == 2, 2 * ONE_WAY + pos, way * ONE_WAY + hop_base + pos)
    slot = (dst_y - src_y) % NY * (NZ * CAP) + src_z * CAP + rank(src * (NY * NZ) + dst)
    turning = join(
        hot(slot, SLOTS, (src_y == my_y) & (dst_z == my_z)), hot(found, 2 * ONE_WAY + OWN)
    )
    place = join(hot(last - me * rows, rows, dst == me), hot(slot, SLOTS))

    counts2d = cluster_member_count.astype(BF).reshape(-1, 128)
    size_last, size_gone = sizes_of(last, counts2d), sizes_of(gone, counts2d)
    retained, selected = size_last / (size_last + size_gone), size_gone / (size_last + size_gone)
    keep, take = row_weights(me * rows, rows, last, gone, retained, selected)
    gone_col, last_col = gone // wcols, last // wcols
    col_rank = rank(gone_col)
    lane = 128
    pick = join(hot(gone - my_col * wcols, wcols), hot(col_rank, lane, gone_col == my_col))

    whole = total // BLOCK * BLOCK
    into = None
    for chunk, (first, end) in enumerate(CHUNKS):
        side = ()
        if chunk == 0:
            side = (jnp.pad(sim_rest[:, whole:], ((0, 0), (0, EDGE - (total - whole)))), sim_window)
        up_list, down_list, own_list = select(sel, sim_rest, side, first, end)
        parts = []
        for step, rows_now in ((1, up_list), (-1, down_list)):
            for hops in HOPS:
                rows_now = lax.ppermute(rows_now[:hops], "row", row_perm(0, step))
                parts.append(rows_now)
        parts.append(own_list)
        ys = turn(turning, parts)
        ys = [ys[0]] + [lax.ppermute(ys[dy], "row", row_perm(dy, 0)) for dy in range(1, NY)]
        outs = blend(place, keep, take, ys, sim_rest, first, end, (sim_window, pick) if side else (), into)
        into = outs[0]
        if side:
            into = lax.dynamic_update_slice(into, outs[1][:, : total - whole], (0, whole))
            mixed, mine = outs[2:]

    pieces = [mine]
    step = 1
    while step < cols_n:
        so_far = jnp.concatenate(pieces, axis=0)
        pieces.append(lax.ppermute(so_far, "col", [(c, c ^ step) for c in range(cols_n)]))
        step *= 2
    spread = join(
        hot((my_col ^ gone_col) * lane + col_rank, cols_n * lane), hot(last - my_col * wcols, wcols)
    )
    ckeep, ctake = item_weights(
        my_col * wcols + jnp.arange(wcols, dtype=jnp.int32), last, gone, retained, selected
    )
    window_out = columns(mixed, ckeep[None, :], ctake[None, :], spread, pieces)
    return window_out, into


def solution(mesh):
    in_specs = (P("row", "col"), P("row", "col"), P(), P())
    out_specs = (P("row", "col"), P("row", "col"))
    return jax.shard_map(shards, mesh=mesh, in_specs=in_specs, out_specs=out_specs, check_vma=False)
```

```python
import functools

import jax
import jax.numpy as jnp
from jax import lax
from jax.experimental import pallas as pl
from jax.experimental.pallas import tpu as pltpu
from jax.sharding import PartitionSpec as P


NY, NZ = 4, 8
SEND = 24
CAP = 3
TO_Z = CAP * NY
SLOTS = NY * NZ * CAP
HALVES = 2
BLOCK = 1280
TILE = 256
Z_ORDER, Y_ORDER = (1, 7, 2, 6, 3, 5, 4), (1, 3, 2)
EDGE = 512
SPLIT = 7680
BF = jnp.bfloat16
F32 = jnp.float32
VMEM = pl.BlockSpec(memory_space=pltpu.VMEM)
ANY = pl.BlockSpec(memory_space=pl.ANY)
HBM = pl.BlockSpec(memory_space=pltpu.HBM)


def row_perm(dy, dz):
    return [
        (y * NZ + z, (y + dy) % NY * NZ + (z + dz) % NZ) for y in range(NY) for z in range(NZ)
    ]


def hot(ids, count, on=None):
    mask = ids[None, :] == jnp.arange(count, dtype=jnp.int32)[:, None]
    if on is not None:
        mask = mask & on[None, :]
    return mask.astype(BF)


def join(left, right):
    return lax.dot_general(left, right, (((1,), (1,)), ((), ())), preferred_element_type=F32).astype(BF)


def joins_kernel(kinds, *refs):
    n = len(refs) // 3
    for (row_halves, col_halves), left, right, out in zip(kinds, refs[:n], refs[n : 2 * n], refs[2 * n :]):
        pairs = left.shape[1]
        rows = lax.broadcasted_iota(jnp.int32, (out.shape[0], pairs), 0) // row_halves
        cols = lax.broadcasted_iota(jnp.int32, (out.shape[1], pairs), 0) // col_halves
        at_row = jnp.where(rows == left[...], 1.0, 0.0).astype(BF)
        at_col = jnp.where(cols == right[...], 1.0, 0.0).astype(BF)
        table = lax.dot_general(at_row, at_col, (((1,), (1,)), ((), ())), preferred_element_type=F32)
        if row_halves > 1 and col_halves > 1:
            row = lax.broadcasted_iota(jnp.int32, table.shape, 0) % HALVES
            col = lax.broadcasted_iota(jnp.int32, table.shape, 1) % HALVES
            table = jnp.where(row == col, table, 0.0)
        out[...] = table.astype(BF)


def joins(*tables):
    pairs = tables[0][1].shape[0]
    shapes = [(rows * rh, cols * ch) for (rows, rh), _, (cols, ch), _ in tables]
    return pl.pallas_call(
        functools.partial(joins_kernel, [(t[0][1], t[2][1]) for t in tables]),
        in_specs=[VMEM] * (2 * len(tables)),
        out_specs=[VMEM] * len(tables),
        out_shape=[jax.ShapeDtypeStruct(s, BF) for s in shapes],
        compiler_params=params(8),
        cost_estimate=pl.CostEstimate(
            flops=sum(2 * r * c * pairs for r, c in shapes), bytes_accessed=0, transcendentals=0
        ),
    )(*[t[1][None, :] for t in tables], *[t[3][None, :] for t in tables])


def rank(code):
    order = jnp.arange(code.shape[0], dtype=jnp.int32)
    same = (code[None, :] == code[:, None]) & (order[None, :] < order[:, None])
    return jnp.sum(same.astype(jnp.int32), axis=1)


def item_weights(labels, lasting, vanishing, retained_pair, selected_pair):
    is_last = labels[:, None] == lasting[None, :]
    is_gone = labels[:, None] == vanishing[None, :]
    matched = jnp.sum((is_last | is_gone).astype(F32), axis=1)
    keep = 1.0 - matched + jnp.sum(jnp.where(is_last, retained_pair[None, :], 0.0), axis=1)
    take = jnp.sum(jnp.where(is_last, selected_pair[None, :], 0.0), axis=1)
    return keep, take


def sizes_of(items, counts2d):
    rows = hot(items // 128, counts2d.shape[0])
    lines = lax.dot_general(rows, counts2d, (((0,), (0,)), ((), ())), preferred_element_type=F32)
    lane = (items % 128)[:, None] == jnp.arange(128, dtype=jnp.int32)[None, :]
    return jnp.sum(jnp.where(lane, lines, 0.0), axis=1)


def params(limit_mib):
    return pltpu.CompilerParams(vmem_limit_bytes=limit_mib * 1024 * 1024)


def tiles(start, width, body):
    count = width // TILE

    @pl.loop(0, count, unroll=next((n for n in (5, 4, 3) if count % n == 0), 1))
    def _(t):
        body(pl.ds(pl.multiple_of(start + t * TILE, TILE), TILE))


def only_half(table, q, axis):
    return jnp.where(lax.broadcasted_iota(jnp.int32, table.shape, axis) % HALVES == q, table, jnp.zeros_like(table))


def edge_pieces(rest, start):
    tail = rest.shape[1] - start
    whole = tail // 128 * 128
    return [(at, width) for at, width in ((0, whole), (whole, tail - whole)) if width]


def pick_halves(sel, x, half, outs):
    first, second = (only_half(sel[...], q, 0) for q in range(HALVES))

    def put(cols):
        later = pl.ds(pl.multiple_of(half + cols.start, TILE), TILE)
        out = jnp.dot(first, x[:, cols], preferred_element_type=F32)
        out += jnp.dot(second, x[:, later], preferred_element_type=F32)
        store_rows(outs, cols, out.astype(BF))

    tiles(0, half, put)


def select_a_kernel(start, main, *refs):
    sel, rest, win = refs[:3]
    outs = refs[3:-3]
    held, tail, sems = refs[-3:]
    side = main + EDGE
    copies = []
    for i, at in enumerate(range(0, main, BLOCK)):
        n = min(BLOCK, main - at)
        copies.append(
            pltpu.make_async_copy(rest.at[:, start + at : start + at + n], held.at[:, at : at + n], sems.at[i])
        )
    copies.append(pltpu.make_async_copy(win, held.at[:, side : side + win.shape[1]], sems.at[len(copies)]))
    copies.append(pltpu.make_async_copy(rest.at[:, start + main :], tail, sems.at[len(copies)]))
    for copy in copies:
        copy.start()
    held[:, main : main + EDGE] = jnp.zeros((held.shape[0], EDGE), BF)
    for copy in copies:
        copy.wait()
    held[:, main : main + tail.shape[1]] = tail[...]
    pick_halves(sel, held, held.shape[1] // HALVES, outs)


def select_a(sel, counts, rest, window, start, main):
    rows = rest.shape[0]
    width = main + EDGE + window.shape[1]
    return pl.pallas_call(
        functools.partial(select_a_kernel, start, main),
        in_specs=[VMEM, HBM, HBM],
        out_specs=[VMEM] * len(counts),
        out_shape=[jax.ShapeDtypeStruct((n, width // HALVES), BF) for n in counts],
        scratch_shapes=[
            pltpu.VMEM((rows, width), BF),
            pltpu.VMEM((rows, rest.shape[1] - start - main), BF),
            pltpu.SemaphoreType.DMA((main // BLOCK + 3,)),
        ],
        compiler_params=params(50),
        cost_estimate=pl.CostEstimate(
            flops=2 * sel.shape[0] * rows * width, bytes_accessed=2 * rows * width, transcendentals=0
        ),
        name="select_a",
    )(sel, rest, window)


def select_b_kernel(sel, rest, out):
    pick_halves(sel, rest, out.shape[1], (out,))


def select_b(sel, rest, width):
    return pl.pallas_call(
        select_b_kernel,
        in_specs=[VMEM] * 2,
        out_specs=VMEM,
        out_shape=jax.ShapeDtypeStruct((sel.shape[0], width // HALVES), BF),
        compiler_params=params(8),
        cost_estimate=pl.CostEstimate(
            flops=2 * sel.size * width, bytes_accessed=2 * rest.shape[0] * width, transcendentals=0
        ),
        name="select_b",
    )(sel, rest)


def weights_kernel(first_row, last, gone, retained, selected, keep, take):
    rows = keep.shape[0]
    label = first_row[0] + lax.broadcasted_iota(jnp.int32, (rows, last.shape[1]), 0)
    is_last, is_gone = label == last[...], label == gone[...]
    kept = jnp.where(is_last, retained[...], jnp.where(is_gone, 0.0, 1.0))
    keep[...] = jnp.min(kept, axis=1, keepdims=True)
    take[...] = jnp.max(jnp.where(is_last, selected[...], 0.0), axis=1, keepdims=True)


def row_weights(first_row, rows, last, gone, retained, selected):
    return pl.pallas_call(
        weights_kernel,
        in_specs=[pl.BlockSpec(memory_space=pltpu.SMEM)] + [VMEM] * 4,
        out_specs=[VMEM] * 2,
        out_shape=[jax.ShapeDtypeStruct((rows, 1), F32)] * 2,
        compiler_params=params(4),
        cost_estimate=pl.CostEstimate(flops=8 * rows * last.shape[0], bytes_accessed=0, transcendentals=0),
        name="row_weights",
    )(first_row[None], last[None, :], gone[None, :], retained[None, :], selected[None, :])


def stack_rows(stack, parts, cols):
    at = 0
    for part in parts:
        stack[at : at + part.shape[0], cols] = part[:, cols]
        at += part.shape[0]


def store_rows(outs, cols, value):
    at = 0
    for out in outs:
        out[:, cols] = value[at : at + out.shape[0]]
        at += out.shape[0]


def turn_kernel(count, *refs):
    sel, parts, outs, stack = refs[0], refs[1 : 1 + count], refs[1 + count : -1], refs[-1]

    def body(cols):
        stack_rows(stack, parts, cols)
        store_rows(outs, cols, jnp.dot(sel[...], stack[:, cols], preferred_element_type=F32).astype(BF))

    tiles(0, stack.shape[1], body)


def turn(sel, parts, counts):
    width = parts[0].shape[1]
    return pl.pallas_call(
        functools.partial(turn_kernel, len(parts)),
        in_specs=[VMEM] * (1 + len(parts)),
        out_specs=[VMEM] * len(counts),
        out_shape=[jax.ShapeDtypeStruct((n, width), BF) for n in counts],
        scratch_shapes=[pltpu.VMEM((sel.shape[1], width), BF)],
        compiler_params=params(8),
        cost_estimate=pl.CostEstimate(
            flops=2 * sel.shape[0] * sel.shape[1] * width, bytes_accessed=sel.size * 2, transcendentals=0
        ),
        name="turn",
    )(sel, *parts)


def blend_kernel(start, main, count, with_side, aliased, *refs):
    place, keep, take, rest = refs[:4]
    ys = refs[4 : 4 + count]
    refs = refs[4 + count :]
    if with_side:
        win, pick = refs[:2]
        refs = refs[2:]
    refs = refs[aliased:]
    if with_side:
        out, mixed, mine, stack, done, sems, edge = refs
    else:
        out, stack, done, sems = refs
    k, t = keep[...], take[...]
    half = stack.shape[1]
    copies = []
    tiles(0, half, lambda cols: stack_rows(stack, ys, cols))
    for q in range(HALVES):
        table = only_half(place[...], q, 1)

        def value(x, at):
            placed = jnp.dot(table, stack[:, pl.ds(at, x.shape[1])], preferred_element_type=F32)
            return (k * x.astype(F32) + t * placed).astype(BF)

        lo, hi = q * half, min((q + 1) * half, main)

        def body(cols, q=q):
            at = pl.multiple_of(cols.start, TILE)
            x = rest[:, pl.ds(pl.multiple_of(start + at, TILE), TILE)]
            done[:, pl.ds(at, TILE)] = value(x, pl.multiple_of(at - q * half, TILE))

        tiles(lo, hi - lo, body)
        copies.append(
            pltpu.make_async_copy(done.at[:, lo:hi], out.at[:, start + lo : start + hi], sems.at[q])
        )
        copies[-1].start()
    if with_side:
        base = main - half
        for at, n in edge_pieces(rest, rest.shape[1] // TILE * TILE):
            x = rest[:, start + main + at : start + main + at + n]
            edge[:, at : at + n] = value(x, base + at)
        copies.append(pltpu.make_async_copy(edge, out.at[:, start + main :], sems.at[HALVES]))
        copies[-1].start()
        for at in range(0, mixed.shape[1], TILE):
            mixed[:, at : at + TILE] = value(win[:, at : at + TILE], base + EDGE + at)
        mine[...] = jnp.dot(mixed[...], pick[...], preferred_element_type=F32).astype(BF)
    for copy in copies:
        copy.wait()


def blend(place, keep, take, ys, rest, start, main, side, into):
    rows, total = rest.shape
    half = ys[0].shape[1]
    with_side, aliased = bool(side), into is not None
    args = [place, keep, take, rest, *ys, *side] + ([into] if aliased else [])
    out_shape, out_specs = [jax.ShapeDtypeStruct((rows, total), BF)], [ANY]
    if with_side:
        out_shape += [jax.ShapeDtypeStruct((rows, n), BF) for n in (side[0].shape[1], side[1].shape[1])]
        out_specs += [VMEM] * 2
    return pl.pallas_call(
        functools.partial(blend_kernel, start, main, len(ys), with_side, aliased),
        in_specs=[VMEM] * (4 + len(ys) + len(side)) + [ANY] * aliased,
        out_specs=out_specs,
        out_shape=out_shape,
        scratch_shapes=[
            pltpu.VMEM((place.shape[1], half), BF),
            pltpu.VMEM((rows, main), BF),
            pltpu.SemaphoreType.DMA((HALVES + 1,)),
        ]
        + ([pltpu.VMEM((rows, total - start - main), BF)] if with_side else []),
        input_output_aliases={len(args) - 1: 0} if aliased else {},
        compiler_params=params(16),
        cost_estimate=pl.CostEstimate(
            flops=4 * place.shape[0] * place.shape[1] * half * HALVES,
            bytes_accessed=2 * rows * half * HALVES,
            transcendentals=0,
        ),
        name="blend",
    )(*args)


def columns_kernel(mixed, keep, take, spread, p0, p1, p2, p3, out, stack, done, sem):
    rows = mixed.shape[0]
    at = 0
    for p in (p0, p1, p2, p3):
        for i in range(p.shape[0] // rows):
            stack[:, at * 128 : (at + 1) * 128] = p[i * rows : (i + 1) * rows, :]
            at += 1

    def body(cols):
        got = jnp.dot(stack[...], spread[:, cols], preferred_element_type=F32)
        done[:, cols] = (keep[:, cols] * mixed[:, cols].astype(F32) + take[:, cols] * got).astype(BF)

    tiles(0, mixed.shape[1], body)
    copy = pltpu.make_async_copy(done, out, sem)
    copy.start()
    copy.wait()


def columns(mixed, keep, take, spread, pieces):
    return pl.pallas_call(
        columns_kernel,
        in_specs=[VMEM] * 8,
        out_specs=ANY,
        out_shape=jax.ShapeDtypeStruct(mixed.shape, BF),
        scratch_shapes=[
            pltpu.VMEM((mixed.shape[0], spread.shape[0]), BF),
            pltpu.VMEM(mixed.shape, BF),
            pltpu.SemaphoreType.DMA,
        ],
        compiler_params=params(8),
        cost_estimate=pl.CostEstimate(
            flops=2 * mixed.size * spread.shape[0], bytes_accessed=2 * mixed.size, transcendentals=0
        ),
        name="columns",
    )(mixed, keep, take, spread, *pieces)


def shards(sim_window, sim_rest, joined_partner_pairs, cluster_member_count):
    rows, wcols = sim_window.shape
    total = sim_rest.shape[1]
    me, my_col = lax.axis_index("row"), lax.axis_index("col")
    cols_n = lax.axis_size("col")
    my_y, my_z = me // NZ, me % NZ
    last, gone = joined_partner_pairs[:, 0], joined_partner_pairs[:, 1]
    src, dst = gone // rows, last // rows
    src_y, src_z, dst_y, dst_z = src // NZ, src % NZ, dst // NZ, dst % NZ
    ahead = (dst_z - src_z) % NZ
    local = jnp.where(src == me, gone - me * rows, -1)
    mine_last = jnp.where(dst == me, last - me * rows, -1)
    to_z = ahead * TO_Z + rank(src * NZ + ahead)
    to_y = (dst_y - src_y) % NY * (NZ * CAP) + src_z * CAP + rank(src * (NY * NZ) + dst)
    list_pos = rank(src)
    in_line = jnp.where((src_z == my_z) & (dst_y == my_y), (my_y - src_y) % NY * SEND + list_pos, -1)
    to_z_b = ahead * TO_Z + rank(src_z * (NY * NZ) + dst)
    two = lambda n: (n, HALVES)
    one = lambda n: (n, 1)
    (sel_a,) = joins((two(SLOTS), to_z, one(rows), local))
    (sel_b,) = joins((two(SEND), list_pos, one(rows), local))
    turn_b, turn_a, place_a, place_b = joins(
        (two(SLOTS), to_z_b, two(SLOTS), in_line),
        (two(SLOTS), to_y, two(SLOTS), jnp.where((src_y == my_y) & (dst_z == my_z), to_z, -1)),
        (one(rows), mine_last, two(SLOTS), to_y),
        (one(rows), mine_last, two(SLOTS), to_z_b),
    )

    counts2d = cluster_member_count.astype(BF).reshape(-1, 128)
    size_last, size_gone = sizes_of(last, counts2d), sizes_of(gone, counts2d)
    retained, selected = size_last / (size_last + size_gone), size_gone / (size_last + size_gone)
    keep, take = row_weights(me * rows, rows, last, gone, retained, selected)
    gone_col = gone // wcols
    col_rank = rank(gone_col)
    lane = 128
    pick = join(hot(gone - my_col * wcols, wcols), hot(col_rank, lane, gone_col == my_col))

    whole = total // TILE * TILE

    def across(lists, along_z):
        got = list(lists)
        for d in Z_ORDER if along_z else Y_ORDER:
            got[d] = lax.ppermute(lists[d], "row", row_perm(0, d) if along_z else row_perm(d, 0))
        return got

    z_counts, y_counts = (TO_Z * HALVES,) * NZ, (SEND * HALVES,) * NY
    lists_a = select_a(sel_a, z_counts, sim_rest, sim_window, SPLIT, whole - SPLIT)
    list_b = select_b(sel_b, sim_rest, SPLIT)
    got_a = across(lists_a, True)
    got_b = across([list_b] * NY, False)
    got_b = across(turn(turn_b, got_b, z_counts), True)
    turned_a = turn(turn_a, got_a, y_counts)
    got_a = across(turned_a, False)

    into, mixed, mine = blend(
        place_a, keep, take, got_a, sim_rest, SPLIT, whole - SPLIT, (sim_window, pick), None
    )
    (rest_out,) = blend(place_b, keep, take, got_b, sim_rest, 0, SPLIT, (), into)

    pieces = [mine]
    step = 1
    while step < cols_n:
        so_far = jnp.concatenate(pieces, axis=0)
        pieces.append(lax.ppermute(so_far, "col", [(c, c ^ step) for c in range(cols_n)]))
        step *= 2
    spread = join(
        hot((my_col ^ gone_col) * lane + col_rank, cols_n * lane), hot(last - my_col * wcols, wcols)
    )
    ckeep, ctake = item_weights(
        my_col * wcols + jnp.arange(wcols, dtype=jnp.int32), last, gone, retained, selected
    )
    window_out = columns(mixed, ckeep[None, :], ctake[None, :], spread, pieces)
    return window_out, rest_out


def solution(mesh):
    in_specs = (P("row", "col"), P("row", "col"), P(), P())
    out_specs = (P("row", "col"), P("row", "col"))

    return jax.shard_map(shards, mesh=mesh, in_specs=in_specs, out_specs=out_specs, check_vma=False)
```

```python
import functools

import jax
import jax.numpy as jnp
from jax import lax
from jax.experimental import pallas as pl
from jax.experimental.pallas import tpu as pltpu
from jax.sharding import PartitionSpec as P


NY, NZ = 4, 8
SEND = 24
CAP = 3
TO_Z = CAP * NY
SLOTS = NY * NZ * CAP
HALVES = 2
BLOCK = 1280
TILE = 256
Z_ORDER, Y_ORDER = (1, 7, 2, 6, 3, 5, 4), (1, 3, 2)
EDGE = 512
SPLIT = 7680
BF = jnp.bfloat16
F32 = jnp.float32
VMEM = pl.BlockSpec(memory_space=pltpu.VMEM)
ANY = pl.BlockSpec(memory_space=pl.ANY)
HBM = pl.BlockSpec(memory_space=pltpu.HBM)


def row_perm(dy, dz):
    return [
        (y * NZ + z, (y + dy) % NY * NZ + (z + dz) % NZ) for y in range(NY) for z in range(NZ)
    ]


def hot(ids, count, on=None):
    mask = ids[None, :] == jnp.arange(count, dtype=jnp.int32)[:, None]
    if on is not None:
        mask = mask & on[None, :]
    return mask.astype(BF)


def join(left, right):
    return lax.dot_general(left, right, (((1,), (1,)), ((), ())), preferred_element_type=F32).astype(BF)


def joins_kernel(kinds, *refs):
    n = len(refs) // 3
    for (row_halves, col_halves), left, right, out in zip(kinds, refs[:n], refs[n : 2 * n], refs[2 * n :]):
        pairs = left.shape[1]
        rows = lax.broadcasted_iota(jnp.int32, (out.shape[0], pairs), 0) // row_halves
        cols = lax.broadcasted_iota(jnp.int32, (out.shape[1], pairs), 0) // col_halves
        at_row = jnp.where(rows == left[...], 1.0, 0.0).astype(BF)
        at_col = jnp.where(cols == right[...], 1.0, 0.0).astype(BF)
        table = lax.dot_general(at_row, at_col, (((1,), (1,)), ((), ())), preferred_element_type=F32)
        if row_halves > 1 and col_halves > 1:
            row = lax.broadcasted_iota(jnp.int32, table.shape, 0) % HALVES
            col = lax.broadcasted_iota(jnp.int32, table.shape, 1) % HALVES
            table = jnp.where(row == col, table, 0.0)
        out[...] = table.astype(BF)


def joins(*tables):
    pairs = tables[0][1].shape[0]
    shapes = [(rows * rh, cols * ch) for (rows, rh), _, (cols, ch), _ in tables]
    return pl.pallas_call(
        functools.partial(joins_kernel, [(t[0][1], t[2][1]) for t in tables]),
        in_specs=[VMEM] * (2 * len(tables)),
        out_specs=[VMEM] * len(tables),
        out_shape=[jax.ShapeDtypeStruct(s, BF) for s in shapes],
        compiler_params=params(8),
        cost_estimate=pl.CostEstimate(
            flops=sum(2 * r * c * pairs for r, c in shapes), bytes_accessed=0, transcendentals=0
        ),
    )(*[t[1][None, :] for t in tables], *[t[3][None, :] for t in tables])


def rank(code):
    order = jnp.arange(code.shape[0], dtype=jnp.int32)
    same = (code[None, :] == code[:, None]) & (order[None, :] < order[:, None])
    return jnp.sum(same.astype(jnp.int32), axis=1)


def item_weights(labels, lasting, vanishing, retained_pair, selected_pair):
    is_last = labels[:, None] == lasting[None, :]
    is_gone = labels[:, None] == vanishing[None, :]
    matched = jnp.sum((is_last | is_gone).astype(F32), axis=1)
    keep = 1.0 - matched + jnp.sum(jnp.where(is_last, retained_pair[None, :], 0.0), axis=1)
    take = jnp.sum(jnp.where(is_last, selected_pair[None, :], 0.0), axis=1)
    return keep, take


def sizes_of(items, counts2d):
    rows = hot(items // 128, counts2d.shape[0])
    lines = lax.dot_general(rows, counts2d, (((0,), (0,)), ((), ())), preferred_element_type=F32)
    lane = (items % 128)[:, None] == jnp.arange(128, dtype=jnp.int32)[None, :]
    return jnp.sum(jnp.where(lane, lines, 0.0), axis=1)


def params(limit_mib):
    return pltpu.CompilerParams(vmem_limit_bytes=limit_mib * 1024 * 1024)


def tiles(start, width, body):
    count = width // TILE

    @pl.loop(0, count, unroll=next((n for n in (5, 4, 3, 7) if count % n == 0), 1))
    def _(t):
        body(pl.ds(pl.multiple_of(start + t * TILE, TILE), TILE))


def only_half(table, q, axis):
    return jnp.where(lax.broadcasted_iota(jnp.int32, table.shape, axis) % HALVES == q, table, jnp.zeros_like(table))


def edge_pieces(rest, start):
    tail = rest.shape[1] - start
    whole = tail // 128 * 128
    return [(at, width) for at, width in ((0, whole), (whole, tail - whole)) if width]


def pick_halves(sel, x, half, outs):
    first, second = (only_half(sel[...], q, 0) for q in range(HALVES))

    def put(cols):
        later = pl.ds(pl.multiple_of(half + cols.start, TILE), TILE)
        out = jnp.dot(first, x[:, cols], preferred_element_type=F32)
        out += jnp.dot(second, x[:, later], preferred_element_type=F32)
        store_rows(outs, cols, out.astype(BF))

    tiles(0, half, put)


def select_a_kernel(start, main, *refs):
    sel, rest, win = refs[:3]
    outs = refs[3:-3]
    held, tail, sems = refs[-3:]
    side = main + EDGE
    copies = []
    for i, at in enumerate(range(0, main, BLOCK)):
        n = min(BLOCK, main - at)
        copies.append(
            pltpu.make_async_copy(rest.at[:, start + at : start + at + n], held.at[:, at : at + n], sems.at[i])
        )
    copies.append(pltpu.make_async_copy(win, held.at[:, side : side + win.shape[1]], sems.at[len(copies)]))
    copies.append(pltpu.make_async_copy(rest.at[:, start + main :], tail, sems.at[len(copies)]))
    for copy in copies:
        copy.start()
    held[:, main : main + EDGE] = jnp.zeros((held.shape[0], EDGE), BF)
    for copy in copies:
        copy.wait()
    held[:, main : main + tail.shape[1]] = tail[...]
    pick_halves(sel, held, held.shape[1] // HALVES, outs)


def select_a(sel, counts, rest, window, start, main):
    rows = rest.shape[0]
    width = main + EDGE + window.shape[1]
    return pl.pallas_call(
        functools.partial(select_a_kernel, start, main),
        in_specs=[VMEM, HBM, HBM],
        out_specs=[VMEM] * len(counts),
        out_shape=[jax.ShapeDtypeStruct((n, width // HALVES), BF) for n in counts],
        scratch_shapes=[
            pltpu.VMEM((rows, width), BF),
            pltpu.VMEM((rows, rest.shape[1] - start - main), BF),
            pltpu.SemaphoreType.DMA((main // BLOCK + 3,)),
        ],
        compiler_params=params(50),
        cost_estimate=pl.CostEstimate(
            flops=2 * sel.shape[0] * rows * width, bytes_accessed=2 * rows * width, transcendentals=0
        ),
        name="select_a",
    )(sel, rest, window)


def select_b_kernel(sel, rest, out):
    pick_halves(sel, rest, out.shape[1], (out,))


def select_b(sel, rest, width):
    return pl.pallas_call(
        select_b_kernel,
        in_specs=[VMEM] * 2,
        out_specs=VMEM,
        out_shape=jax.ShapeDtypeStruct((sel.shape[0], width // HALVES), BF),
        compiler_params=params(8),
        cost_estimate=pl.CostEstimate(
            flops=2 * sel.size * width, bytes_accessed=2 * rest.shape[0] * width, transcendentals=0
        ),
        name="select_b",
    )(sel, rest)


def weights_kernel(first_row, last, gone, retained, selected, keep, take):
    rows = keep.shape[0]
    label = first_row[0] + lax.broadcasted_iota(jnp.int32, (rows, last.shape[1]), 0)
    is_last, is_gone = label == last[...], label == gone[...]
    kept = jnp.where(is_last, retained[...], jnp.where(is_gone, 0.0, 1.0))
    keep[...] = jnp.min(kept, axis=1, keepdims=True)
    take[...] = jnp.max(jnp.where(is_last, selected[...], 0.0), axis=1, keepdims=True)


def row_weights(first_row, rows, last, gone, retained, selected):
    return pl.pallas_call(
        weights_kernel,
        in_specs=[pl.BlockSpec(memory_space=pltpu.SMEM)] + [VMEM] * 4,
        out_specs=[VMEM] * 2,
        out_shape=[jax.ShapeDtypeStruct((rows, 1), F32)] * 2,
        compiler_params=params(4),
        cost_estimate=pl.CostEstimate(flops=8 * rows * last.shape[0], bytes_accessed=0, transcendentals=0),
        name="row_weights",
    )(first_row[None], last[None, :], gone[None, :], retained[None, :], selected[None, :])


def stack_rows(stack, parts, cols):
    at = 0
    for part in parts:
        stack[at : at + part.shape[0], cols] = part[:, cols]
        at += part.shape[0]


def store_rows(outs, cols, value):
    at = 0
    for out in outs:
        out[:, cols] = value[at : at + out.shape[0]]
        at += out.shape[0]


def turn_kernel(count, *refs):
    sel, parts, outs, stack = refs[0], refs[1 : 1 + count], refs[1 + count : -1], refs[-1]

    def body(cols):
        stack_rows(stack, parts, cols)
        store_rows(outs, cols, jnp.dot(sel[...], stack[:, cols], preferred_element_type=F32).astype(BF))

    tiles(0, stack.shape[1], body)


def turn(sel, parts, counts):
    width = parts[0].shape[1]
    return pl.pallas_call(
        functools.partial(turn_kernel, len(parts)),
        in_specs=[VMEM] * (1 + len(parts)),
        out_specs=[VMEM] * len(counts),
        out_shape=[jax.ShapeDtypeStruct((n, width), BF) for n in counts],
        scratch_shapes=[pltpu.VMEM((sel.shape[1], width), BF)],
        compiler_params=params(8),
        cost_estimate=pl.CostEstimate(
            flops=2 * sel.shape[0] * sel.shape[1] * width, bytes_accessed=sel.size * 2, transcendentals=0
        ),
        name="turn",
    )(sel, *parts)


def blend_kernel(start, main, count, with_side, aliased, *refs):
    place, keep, take, rest = refs[:4]
    ys = refs[4 : 4 + count]
    refs = refs[4 + count :]
    if with_side:
        win, pick = refs[:2]
        refs = refs[2:]
    refs = refs[aliased:]
    if with_side:
        out, mixed, mine, stack, done, sems, edge = refs
    else:
        out, stack, done, sems = refs
    k, t = keep[...], take[...]
    half = stack.shape[1]
    copies = []
    tiles(0, half, lambda cols: stack_rows(stack, ys, cols))
    for q in range(HALVES):
        table = only_half(place[...], q, 1)

        def value(x, at):
            placed = jnp.dot(table, stack[:, pl.ds(at, x.shape[1])], preferred_element_type=F32)
            return (k * x.astype(F32) + t * placed).astype(BF)

        lo, hi = q * half, min((q + 1) * half, main)

        def body(cols, q=q):
            at = pl.multiple_of(cols.start, TILE)
            x = rest[:, pl.ds(pl.multiple_of(start + at, TILE), TILE)]
            done[:, pl.ds(at, TILE)] = value(x, pl.multiple_of(at - q * half, TILE))

        tiles(lo, hi - lo, body)
        copies.append(
            pltpu.make_async_copy(done.at[:, lo:hi], out.at[:, start + lo : start + hi], sems.at[q])
        )
        copies[-1].start()
    if with_side:
        base = main - half
        for at, n in edge_pieces(rest, rest.shape[1] // TILE * TILE):
            x = rest[:, start + main + at : start + main + at + n]
            edge[:, at : at + n] = value(x, base + at)
        copies.append(pltpu.make_async_copy(edge, out.at[:, start + main :], sems.at[HALVES]))
        copies[-1].start()
        for at in range(0, mixed.shape[1], TILE):
            mixed[:, at : at + TILE] = value(win[:, at : at + TILE], base + EDGE + at)
        mine[...] = jnp.dot(mixed[...], pick[...], preferred_element_type=F32).astype(BF)
    for copy in copies:
        copy.wait()


def blend(place, keep, take, ys, rest, start, main, side, into):
    rows, total = rest.shape
    half = ys[0].shape[1]
    with_side, aliased = bool(side), into is not None
    args = [place, keep, take, rest, *ys, *side] + ([into] if aliased else [])
    out_shape, out_specs = [jax.ShapeDtypeStruct((rows, total), BF)], [ANY]
    if with_side:
        out_shape += [jax.ShapeDtypeStruct((rows, n), BF) for n in (side[0].shape[1], side[1].shape[1])]
        out_specs += [VMEM] * 2
    return pl.pallas_call(
        functools.partial(blend_kernel, start, main, len(ys), with_side, aliased),
        in_specs=[VMEM] * (4 + len(ys) + len(side)) + [ANY] * aliased,
        out_specs=out_specs,
        out_shape=out_shape,
        scratch_shapes=[
            pltpu.VMEM((place.shape[1], half), BF),
            pltpu.VMEM((rows, main), BF),
            pltpu.SemaphoreType.DMA((HALVES + 1,)),
        ]
        + ([pltpu.VMEM((rows, total - start - main), BF)] if with_side else []),
        input_output_aliases={len(args) - 1: 0} if aliased else {},
        compiler_params=params(16),
        cost_estimate=pl.CostEstimate(
            flops=4 * place.shape[0] * place.shape[1] * half * HALVES,
            bytes_accessed=2 * rows * half * HALVES,
            transcendentals=0,
        ),
        name="blend",
    )(*args)


def columns_kernel(mixed, keep, take, spread, *refs):
    pieces, (out, stack, done, sem) = refs[:-4], refs[-4:]
    rows = mixed.shape[0]
    at = 0
    for p in pieces:
        for i in range(p.shape[0] // rows):
            stack[:, at * 128 : (at + 1) * 128] = p[i * rows : (i + 1) * rows, :]
            at += 1

    def body(cols):
        got = jnp.dot(stack[...], spread[:, cols], preferred_element_type=F32)
        done[:, cols] = (keep[:, cols] * mixed[:, cols].astype(F32) + take[:, cols] * got).astype(BF)

    tiles(0, mixed.shape[1], body)
    copy = pltpu.make_async_copy(done, out, sem)
    copy.start()
    copy.wait()


def columns(mixed, keep, take, spread, pieces):
    return pl.pallas_call(
        columns_kernel,
        in_specs=[VMEM] * (4 + len(pieces)),
        out_specs=ANY,
        out_shape=jax.ShapeDtypeStruct(mixed.shape, BF),
        scratch_shapes=[
            pltpu.VMEM((mixed.shape[0], spread.shape[0]), BF),
            pltpu.VMEM(mixed.shape, BF),
            pltpu.SemaphoreType.DMA,
        ],
        compiler_params=params(8),
        cost_estimate=pl.CostEstimate(
            flops=2 * mixed.size * spread.shape[0], bytes_accessed=2 * mixed.size, transcendentals=0
        ),
        name="columns",
    )(mixed, keep, take, spread, *pieces)


def shards(sim_window, sim_rest, joined_partner_pairs, cluster_member_count):
    rows, wcols = sim_window.shape
    total = sim_rest.shape[1]
    me, my_col = lax.axis_index("row"), lax.axis_index("col")
    cols_n = lax.axis_size("col")
    my_y, my_z = me // NZ, me % NZ
    last, gone = joined_partner_pairs[:, 0], joined_partner_pairs[:, 1]
    src, dst = gone // rows, last // rows
    src_y, src_z, dst_y, dst_z = src // NZ, src % NZ, dst // NZ, dst % NZ
    ahead = (dst_z - src_z) % NZ
    local = jnp.where(src == me, gone - me * rows, -1)
    mine_last = jnp.where(dst == me, last - me * rows, -1)
    to_z = ahead * TO_Z + rank(src * NZ + ahead)
    to_y = (dst_y - src_y) % NY * (NZ * CAP) + src_z * CAP + rank(src * (NY * NZ) + dst)
    list_pos = rank(src)
    in_line = jnp.where((src_z == my_z) & (dst_y == my_y), (my_y - src_y) % NY * SEND + list_pos, -1)
    to_z_b = ahead * TO_Z + rank(src_z * (NY * NZ) + dst)
    two = lambda n: (n, HALVES)
    one = lambda n: (n, 1)
    (sel_a,) = joins((two(SLOTS), to_z, one(rows), local))
    (sel_b,) = joins((two(SEND), list_pos, one(rows), local))
    turn_b, turn_a, place_a, place_b = joins(
        (two(SLOTS), to_z_b, two(SLOTS), in_line),
        (two(SLOTS), to_y, two(SLOTS), jnp.where((src_y == my_y) & (dst_z == my_z), to_z, -1)),
        (one(rows), mine_last, two(SLOTS), to_y),
        (one(rows), mine_last, two(SLOTS), to_z_b),
    )

    counts2d = cluster_member_count.astype(BF).reshape(-1, 128)
    size_last, size_gone = sizes_of(last, counts2d), sizes_of(gone, counts2d)
    retained, selected = size_last / (size_last + size_gone), size_gone / (size_last + size_gone)
    keep, take = row_weights(me * rows, rows, last, gone, retained, selected)
    gone_col = gone // wcols
    col_rank = rank(gone_col)
    lane = 128
    pick = join(hot(gone - my_col * wcols, wcols), hot(col_rank, lane, gone_col == my_col))

    whole = total // TILE * TILE

    def across(lists, along_z):
        got = list(lists)
        for d in Z_ORDER if along_z else Y_ORDER:
            got[d] = lax.ppermute(lists[d], "row", row_perm(0, d) if along_z else row_perm(d, 0))
        return got

    z_counts, y_counts = (TO_Z * HALVES,) * NZ, (SEND * HALVES,) * NY
    lists_a = select_a(sel_a, z_counts, sim_rest, sim_window, SPLIT, whole - SPLIT)
    list_b = select_b(sel_b, sim_rest, SPLIT)
    got_a = across(lists_a, True)
    got_b = across([list_b] * NY, False)
    got_b = across(turn(turn_b, got_b, z_counts), True)
    turned_a = turn(turn_a, got_a, y_counts)
    got_a = across(turned_a, False)

    into, mixed, mine = blend(
        place_a, keep, take, got_a, sim_rest, SPLIT, whole - SPLIT, (sim_window, pick), None
    )
    (rest_out,) = blend(place_b, keep, take, got_b, sim_rest, 0, SPLIT, (), into)

    def crossed(piece, k):
        return lax.ppermute(piece, "col", [(c, c ^ k) for c in range(cols_n)])

    both = jnp.concatenate([mine, crossed(mine, 1)], axis=0)
    pieces = [both] + [crossed(both, k) for k in range(2, cols_n, 2)]
    spread = join(
        hot((my_col ^ gone_col) * lane + col_rank, cols_n * lane), hot(last - my_col * wcols, wcols)
    )
    ckeep, ctake = item_weights(
        my_col * wcols + jnp.arange(wcols, dtype=jnp.int32), last, gone, retained, selected
    )
    window_out = columns(mixed, ckeep[None, :], ctake[None, :], spread, pieces)
    return window_out, rest_out


def solution(mesh):
    in_specs = (P("row", "col"), P("row", "col"), P(), P())
    out_specs = (P("row", "col"), P("row", "col"))

    return jax.shard_map(shards, mesh=mesh, in_specs=in_specs, out_specs=out_specs, check_vma=False)
```
